32 devices in a mesh: expert: 8 (over z, x), shard: 4 (over y, core).
Axes of the slice: x: 2, y: 2, z: 4, core: 2. Of those that a mesh axis runs over, the one named last changes fastest.
Arguments:
- tokens: bfloat16 [160, 197, 512], P(('expert', 'shard')), may hold values from -6 to 6
- attn_gain: float32 [512], replicated, may hold values from 0.5 to 1.5
- moe_gain: float32 [512], replicated, may hold values from 0.5 to 1.5
- qkv_weight: bfloat16 [512, 1536], P('shard'), may hold values from -0.25 to 0.25
- out_weight: bfloat16 [512, 512], P('shard'), may hold values from -0.5 to 0.5
- router_weight: bfloat16 [512, 8], P('shard'), may hold values from -0.25 to 0.25
- up_weight: bfloat16 [8, 512, 2048], P('expert', None, 'shard'), may hold values from -0.25 to 0.25
- down_weight: bfloat16 [8, 2048, 512], P('expert', 'shard'), may hold values from -0.5 to 0.5
- qkv_left: bfloat16 [512, 384], P('shard'), may hold values from -0.25 to 0.25
- qkv_right: bfloat16 [3, 128, 512], P(None, 'shard'), may hold values from -0.75 to 0.75
- out_left: bfloat16 [512, 128], P('shard'), may hold values from -0.25 to 0.25
- out_right: bfloat16 [128, 512], P('shard'), may hold values from -1.5 to 1.5
- router_left: bfloat16 [512, 128], P('shard'), may hold values from -0.25 to 0.25
- router_right: bfloat16 [128, 8], P('shard'), may hold values from -0.75 to 0.75
- up_left: bfloat16 [8, 512, 128], P('expert', 'shard'), may hold values from -0.25 to 0.25
- up_right: bfloat16 [8, 128, 2048], P('expert', None, 'shard'), may hold values from -0.75 to 0.75
- down_left: bfloat16 [8, 2048, 128], P('expert', 'shard'), may hold values from -0.125 to 0.125
- down_right: bfloat16 [8, 128, 512], P('expert', None, 'shard'), may hold values from -1.5 to 1.5
- routes: int32 [160, 197, 2], P(('expert', 'shard')), may hold values from 0 to 7, as said below
- capacity: int32 [8], replicated, may hold values from 156 to 312, as said below
- adapter_id: int32 [160], P(('expert', 'shard')), may hold values from 0 to 7
- cotangent: bfloat16 [160, 197, 512], P(('expert', 'shard')), may hold values from -6 to 6
Outputs:
- layer_out: bfloat16 [160, 197, 512], P(('expert', 'shard'))
- tokens_grad: float32 [160, 197, 512], P(('expert', 'shard'))
- qleft_grad: float32 [512, 384], P('shard')
- qright_grad: float32 [3, 128, 512], P(None, 'shard')
- oleft_grad: float32 [512, 128], P('shard')
- oright_grad: float32 [128, 512], P('shard')
- rleft_grad: float32 [512, 128], P('shard')
- rright_grad: float32 [128, 8], P('shard')
- uleft_grad: float32 [8, 512, 128], P('expert', 'shard')
- uright_grad: float32 [8, 128, 2048], P('expert', None, 'shard')
- dleft_grad: float32 [8, 2048, 128], P('expert', 'shard')
- dright_grad: float32 [8, 128, 512], P('expert', None, 'shard')
The draws below stay inside these ranges and needn't reach their ends.
Inputs may be any that keep to these rules, and one draw needn't show every extreme that they name: `routes`: each token names two different experts. One expert has capacity 312.
All inputs are finite; a program needn't handle non-finite values.
Results may differ from the reference program's by a relative error of at most 0.022.
Values may be sent and summed in bfloat16 or wider, within the bound.
A program may use at most 256 MiB of HBM per device.

```python
import jax
import jax.numpy as jnp
from jax import lax

D = 512
HEADS = 8
HEAD_DIM = 64
FF = 2048
SEQ = 197
ADAPTERS = 8
RANK = 16
IMG_DEV = 5
EXPERTS = 8
IMAGES = 160
ADAPT_COLS = 128
CAP = 312


def expert_order(key):
    return jax.random.permutation(jax.random.fold_in(key, 11), EXPERTS).astype(jnp.int32)


def draw_routes(key, part):
    order = expert_order(key)
    shape = (IMAGES, SEQ)
    first_pick = jax.random.randint(jax.random.fold_in(key, 1), shape, 0, EXPERTS)
    second_pick = jax.random.randint(jax.random.fold_in(key, 2), shape, 0, EXPERTS)
    third_pick = jax.random.randint(jax.random.fold_in(key, 3), shape, 0, EXPERTS)
    leading = order[jnp.minimum(jnp.minimum(first_pick, second_pick), third_pick)]
    offset = jax.random.randint(jax.random.fold_in(key, 4), shape, 1, EXPERTS)
    other = (leading + offset) % EXPERTS
    return jnp.stack([leading, other], axis=-1).astype(jnp.int32)


def draw_capacity(key, part):
    order = expert_order(key)
    drawn = jax.random.randint(jax.random.fold_in(key, 5), (EXPERTS,), CAP // 2, CAP + 1)
    return jnp.where(jnp.arange(EXPERTS, dtype=jnp.int32) == order[0], CAP, drawn).astype(jnp.int32)


def touch_ends(values, own_key, smallest, high):
    extent = values.shape
    spot = [jax.random.randint(jax.random.fold_in(own_key, axis), (), 0, extent[axis]) for axis in range(len(extent))]
    values = values.at[tuple(spot)].set(smallest)
    longest = extent.index(max(extent))
    spot[longest] = (spot[longest] + 1) % extent[longest]
    return values.at[tuple(spot)].set(high)


def block_scale(rng, dims, shards, least, largest):
    level, own = 1.0, jax.random.fold_in(rng, 6)
    for dim, blocks in shards:
        steps = jnp.exp(jax.random.uniform(jax.random.fold_in(own, dim), (blocks,), jnp.float32, least / len(shards), largest / len(shards)))
        level = level * jnp.repeat(steps, dims[dim] // blocks).reshape([-1 if axis == dim else 1 for axis in range(len(dims))])
    return level


def bell_draw(rng, shape, spread, bound, split=(), held_as=jnp.bfloat16):
    values = jax.random.normal(rng, shape, jnp.float32) * spread
    if len(split) > 0:
        values = block_scale(rng, shape, split, -0.22, 0.18) * values
    return jnp.clip(values, min=-bound, max=bound).astype(held_as)


def setup_inputs(seed: int = 0) -> dict:
    key_of = jax.random.split(jax.random.key(seed), 23)
    return {
        "tokens": bell_draw(key_of[0], (IMAGES, SEQ, D), 1.0, 6.0, ((0, 32),)),
        "attn_gain": jnp.clip(1.0 + 0.1 * jax.random.normal(key_of[1], (D,), jnp.float32), 0.5, 1.5),
        "moe_gain": jnp.clip(1.0 + 0.1 * jax.random.normal(key_of[2], (D,), jnp.float32), 0.5, 1.5),
        "qkv_weight": bell_draw(key_of[3], (D, 3 * D), D ** -0.5, 0.25, ((0, 4),)),
        "out_weight": bell_draw(key_of[4], (D, D), (D // 4) ** -0.5, 0.5, ((0, 4),)),
        "router_weight": bell_draw(key_of[5], (D, EXPERTS), D ** -0.5, 0.25, ((0, 4),)),
        "up_weight": bell_draw(key_of[6], (EXPERTS, D, FF), D ** -0.5, 0.25, ((0, 8), (2, 4))),
        "down_weight": bell_draw(key_of[7], (EXPERTS, FF, D), (FF // 16) ** -0.5, 0.5, ((0, 8), (1, 4))),
        "qkv_left": bell_draw(key_of[8], (D, 3 * ADAPT_COLS), D ** -0.5, 0.25, ((0, 4),)),
        "qkv_right": bell_draw(key_of[9], (3, ADAPT_COLS, D), (RANK * 4) ** -0.5, 0.75, ((1, 4),)),
        "out_left": bell_draw(key_of[10], (D, ADAPT_COLS), D ** -0.5, 0.25, ((0, 4),)),
        "out_right": bell_draw(key_of[11], (ADAPT_COLS, D), RANK ** -0.5, 1.5, ((0, 4),)),
        "router_left": bell_draw(key_of[12], (D, ADAPT_COLS), D ** -0.5, 0.25, ((0, 4),)),
        "router_right": bell_draw(key_of[13], (ADAPT_COLS, EXPERTS), (RANK * 4) ** -0.5, 0.75, ((0, 4),)),
        "up_left": bell_draw(key_of[14], (EXPERTS, D, ADAPT_COLS), D ** -0.5, 0.25, ((0, 8), (1, 4))),
        "up_right": bell_draw(key_of[15], (EXPERTS, ADAPT_COLS, FF), (RANK * 4) ** -0.5, 0.75, ((0, 8), (2, 4))),
        "down_left": bell_draw(key_of[16], (EXPERTS, FF, ADAPT_COLS), FF ** -0.5, 0.125, ((0, 8), (1, 4))),
        "down_right": bell_draw(key_of[17], (EXPERTS, ADAPT_COLS, D), RANK ** -0.5, 1.5, ((0, 8), (2, 4))),
        "routes": draw_routes(jax.random.fold_in(key_of[22], 71), 0),
        "capacity": draw_capacity(jax.random.fold_in(key_of[22], 71), 0),
        "adapter_id": touch_ends(jax.random.randint(key_of[20], (IMAGES,), 0, ADAPTERS), jax.random.fold_in(key_of[20], 1), 0, ADAPTERS - 1).astype(jnp.int32),
        "cotangent": bell_draw(key_of[21], (IMAGES, SEQ, D), 1.0, 6.0, ((0, 32),)),
    }


HIGHEST = lax.Precision.HIGHEST
EPSILON = 1e-06

@jax.custom_vjp
def low(v):
    return lax.optimization_barrier(v.astype(jnp.bfloat16)).astype(jnp.float32)

@jax.custom_vjp
def low_back(v):
    return v

def low_keep(v):
    return (low(v), None)

def low_pass(kept, grad):
    return (grad,)

def back_keep(v):
    return (v, None)

def back_low(kept, grad):
    return (low(grad),)
low.defvjp(low_keep, low_pass)
low_back.defvjp(back_keep, back_low)

def dense(left, right):
    return jnp.dot(left, right, precision=HIGHEST, preferred_element_type=jnp.float32)

def layer_norm(values, gain):
    centred = values - lax.optimization_barrier(jnp.mean(values, axis=-1, keepdims=True))
    inverse = lax.rsqrt(lax.optimization_barrier(jnp.mean(centred * centred, axis=-1, keepdims=True)) + EPSILON)
    return centred * inverse * gain

def attention_group(group_rows, group_mask, gain, qkv_weight, out_weight, qkv_left, qkv_right, out_left, out_right):
    flat_rows = group_rows.reshape(-1, D)
    token_mask = jnp.repeat(group_mask, SEQ, axis=0)
    normed = low(layer_norm(flat_rows, gain))
    qkv_low = low_back(low(dense(normed, qkv_left))).reshape(-1, 3, ADAPT_COLS) * token_mask[:, None, :]
    qkv_delta = jnp.einsum('tjr,jrd->tjd', qkv_low, qkv_right, precision=HIGHEST).reshape(-1, 3 * D)
    qkv_rows = low_back(low(dense(normed, qkv_weight) + qkv_delta))
    qkv_split = qkv_rows.reshape(-1, SEQ, 3, HEADS, HEAD_DIM)
    queries = qkv_split[:, :, 0]
    key_rows = qkv_split[:, :, 1]
    value_rows = qkv_split[:, :, 2]
    scores = low_back(jnp.einsum('bqhd,bkhd->bhqk', queries, key_rows, precision=HIGHEST) * HEAD_DIM ** (-0.5))
    weights_low = low(jax.nn.softmax(scores, axis=-1))
    attended = jnp.einsum('bhqk,bkhd->bqhd', weights_low, value_rows, precision=HIGHEST).reshape(-1, D)
    attended = low_back(low(attended))
    out_low = low_back(low(dense(attended, out_left))) * token_mask
    attn_rows = low_back(dense(attended, out_weight) + dense(out_low, out_right))
    return (flat_rows + attn_rows).reshape(group_rows.shape)

def moe_group(group_rows, group_mask, group_routes, capacity, gain, router_weight, up_weight, down_weight, router_left, router_right, up_left, up_right, down_left, down_right):
    flat_rows = group_rows.reshape(-1, D)
    token_count = flat_rows.shape[0]
    token_mask = jnp.repeat(group_mask, SEQ, axis=0)
    normed = low(layer_norm(flat_rows, gain))
    router_low = low_back(low(dense(normed, router_left))) * token_mask
    logits = low_back(dense(normed, router_weight) + dense(router_low, router_right))
    router_probs = jax.nn.softmax(logits, axis=-1)
    pair_routes = group_routes.reshape(token_count, 2).T.reshape(-1)
    expert_hot = (pair_routes[:, None] == jnp.arange(EXPERTS, dtype=jnp.int32)[None, :]).astype(jnp.int32)
    place = lax.optimization_barrier(jnp.sum((jnp.cumsum(expert_hot, axis=0) - 1) * expert_hot, axis=1))
    limit = lax.optimization_barrier(jnp.sum(expert_hot * capacity[None, :], axis=1))
    kept = place < limit
    slot_index = jnp.where(kept, pair_routes * CAP + place, EXPERTS * CAP).astype(jnp.int32)
    pair_ids = jnp.arange(2 * token_count, dtype=jnp.int32)
    source = jnp.full((EXPERTS * CAP + 1,), 2 * token_count, jnp.int32).at[slot_index].set(pair_ids)[:EXPERTS * CAP]
    token_index = jnp.where(source < 2 * token_count, source % token_count, token_count).astype(jnp.int32)
    normed_padded = jnp.concatenate([normed, jnp.zeros((1, D), jnp.float32)], axis=0)
    mask_padded = jnp.concatenate([token_mask, jnp.zeros((1, ADAPT_COLS), jnp.float32)], axis=0)
    sent_rows = low_back(normed_padded[token_index]).reshape(EXPERTS, CAP, D)
    slot_mask = mask_padded[token_index].reshape(EXPERTS, CAP, ADAPT_COLS)
    expert_low = low(jnp.einsum('ecd,edr->ecr', sent_rows, up_left, precision=HIGHEST)) * slot_mask
    pre_act = low_back(jnp.einsum('ecd,edf->ecf', sent_rows, up_weight, precision=HIGHEST) + jnp.einsum('ecr,erf->ecf', expert_low, up_right, precision=HIGHEST))
    hidden = low(jax.nn.gelu(pre_act, approximate=False))
    down_low = low_back(jnp.einsum('ecf,efr->ecr', hidden, down_left, precision=HIGHEST)) * slot_mask
    expert_rows = jnp.einsum('ecf,efd->ecd', hidden, down_weight, precision=HIGHEST) + jnp.einsum('ecr,erd->ecd', down_low, down_right, precision=HIGHEST)
    expert_rows = low_back(low(expert_rows))
    flat_out = jnp.concatenate([expert_rows.reshape(-1, D), jnp.zeros((1, D), jnp.float32)], axis=0)
    picked = flat_out[slot_index]
    pair_probs = jnp.concatenate([router_probs, router_probs], axis=0)
    gate = lax.optimization_barrier(jnp.sum(pair_probs * expert_hot.astype(jnp.float32), axis=1)) * kept.astype(jnp.float32)
    weighted = (gate[:, None] * picked).reshape(2, token_count, D)
    return (flat_rows + weighted[0] + weighted[1]).reshape(group_rows.shape)

def reference(tokens, attn_gain, moe_gain, qkv_weight, out_weight, router_weight, up_weight, down_weight, qkv_left, qkv_right, out_left, out_right, router_left, router_right, up_left, up_right, down_left, down_right, routes, capacity, adapter_id, cotangent):
    groups = IMAGES // IMG_DEV
    image_mask = ((jnp.arange(ADAPT_COLS, dtype=jnp.int32) // RANK)[None, :] == adapter_id[:, None]).astype(jnp.float32)
    mask_groups = image_mask.reshape(groups, IMG_DEV, ADAPT_COLS)
    route_groups = routes.reshape(groups, IMG_DEV, SEQ, 2)
    qkv_full = qkv_weight.astype(jnp.float32)
    out_full = out_weight.astype(jnp.float32)
    router_full = router_weight.astype(jnp.float32)
    up_full = up_weight.astype(jnp.float32)
    down_full = down_weight.astype(jnp.float32)

    def forward(inputs, q_left, q_right, o_left, o_right, r_left, r_right, u_left, u_right, d_left, d_right):
        grouped = inputs.reshape(groups, IMG_DEV, SEQ, D)

        def attend(pieces):
            return attention_group(pieces[0], pieces[1], attn_gain, qkv_full, out_full, q_left, q_right, o_left, o_right)
        after_attn = lax.map(jax.checkpoint(attend), (grouped, mask_groups))

        def mixture(pieces):
            return moe_group(pieces[0], pieces[1], pieces[2], capacity, moe_gain, router_full, up_full, down_full, r_left, r_right, u_left, u_right, d_left, d_right)
        return lax.map(jax.checkpoint(mixture), (after_attn, mask_groups, route_groups)).reshape(IMAGES, SEQ, D)
    primals = tuple((array.astype(jnp.float32) for array in (tokens, qkv_left, qkv_right, out_left, out_right, router_left, router_right, up_left, up_right, down_left, down_right)))
    final_sum, pull_back = jax.vjp(forward, *primals)
    grads = pull_back(cotangent.astype(jnp.float32))
    return (final_sum.astype(jnp.bfloat16), grads[0], grads[1], grads[2], grads[3], grads[4], grads[5], grads[6], grads[7], grads[8], grads[9], grads[10])
```

```python
import functools

import jax
import jax.numpy as jnp
from jax import lax
from jax.experimental import pallas as pl
from jax.experimental.pallas import tpu as pltpu
from jax.sharding import PartitionSpec as P


D = 512
HEADS = 8
HEAD_DIM = 64
SEQ = 197
ADAPTERS = 8
RANK = 16
ADAPT_COLS = 128


HIGHEST = lax.Precision.HIGHEST
EPSILON = 1e-06


def slot_count(token_count, experts):
    return max(8, (2 * token_count * 5 // 4 // experts + 7) // 8 * 8)


def product(left, right):
    return jnp.dot(left, right, preferred_element_type=jnp.float32)


def cross_rows(left, right):
    return jnp.dot(left.T, right, preferred_element_type=jnp.float32)


def back_rows(left, right):
    return jnp.dot(left, right.T, preferred_element_type=jnp.float32)


def layer_norm(values, gain):
    centred = values - jnp.mean(values, axis=-1, keepdims=True)
    inverse = lax.rsqrt(jnp.mean(centred * centred, axis=-1, keepdims=True) + EPSILON)
    normal = centred * inverse
    return (normal * gain, normal, inverse)


def norm_back(grad_in, gain, normal, inverse):
    scaled = grad_in * gain
    return inverse * (
        scaled
        - jnp.mean(scaled, axis=-1, keepdims=True)
        - normal * jnp.mean(scaled * normal, axis=-1, keepdims=True)
    )


def gelu_exact(value):
    return jax.nn.gelu(value, approximate=False)


def expert_forward(
    rows_in, mask_cols, weight_up, weight_down, left_up, right_up, left_down, right_down
):
    expert_low = (
        jnp.einsum("sjcd,jdr->sjcr", rows_in, left_up, preferred_element_type=jnp.float32).astype(
            jnp.bfloat16
        )
        * mask_cols
    )
    pre_act = jnp.einsum(
        "sjcd,jdf->sjcf", rows_in, weight_up, preferred_element_type=jnp.float32
    ) + jnp.einsum("sjcr,jrf->sjcf", expert_low, right_up, preferred_element_type=jnp.float32)
    hidden = gelu_exact(pre_act).astype(jnp.bfloat16)
    down_low = jnp.einsum(
        "sjcf,jfr->sjcr", hidden, left_down, preferred_element_type=jnp.float32
    ) * mask_cols.astype(jnp.float32)
    result = jnp.einsum(
        "sjcf,jfd->sjcd", hidden, weight_down, preferred_element_type=jnp.float32
    ) + jnp.einsum("sjcr,jrd->sjcd", down_low, right_down.astype(jnp.float32), precision=HIGHEST)
    return (result, (expert_low, pre_act, hidden, down_low))


def expert_backward(
    rows_in,
    mask_cols,
    grad_rows,
    saved,
    weight_up,
    weight_down,
    left_up,
    right_up,
    left_down,
    right_down,
):
    expert_low, pre_act, hidden, down_low = saved
    mask_wide = mask_cols.astype(jnp.float32)
    dright = jnp.einsum(
        "sjcr,sjcd->jrd", down_low, grad_rows.astype(jnp.float32), precision=HIGHEST
    )
    down_grad = (
        jnp.einsum("sjcd,jrd->sjcr", grad_rows, right_down, preferred_element_type=jnp.float32)
        * mask_wide
    ).astype(jnp.bfloat16)
    dleft = jnp.einsum("sjcf,sjcr->jfr", hidden, down_grad, preferred_element_type=jnp.float32)
    hidden_grad = jnp.einsum(
        "sjcd,jfd->sjcf", grad_rows, weight_down, preferred_element_type=jnp.float32
    ) + jnp.einsum("sjcr,jfr->sjcf", down_grad, left_down, preferred_element_type=jnp.float32)
    activation, pull_back = jax.vjp(gelu_exact, pre_act)
    pre_grad = pull_back(hidden_grad)[0].astype(jnp.bfloat16)
    uright = jnp.einsum("sjcr,sjcf->jrf", expert_low, pre_grad, preferred_element_type=jnp.float32)
    up_grad = (
        jnp.einsum("sjcf,jrf->sjcr", pre_grad, right_up, preferred_element_type=jnp.float32)
        * mask_wide
    )
    uleft = jnp.einsum("sjcd,sjcr->jdr", rows_in.astype(jnp.float32), up_grad, precision=HIGHEST)
    rows_grad = jnp.einsum(
        "sjcf,jdf->sjcd", pre_grad, weight_up, preferred_element_type=jnp.float32
    ) + jnp.einsum("sjcr,jdr->sjcd", up_grad, left_up.astype(jnp.float32), precision=HIGHEST)
    return (rows_grad, (uleft, uright, dleft, dright))


def general_path(
    tokens,
    attn_gain,
    moe_gain,
    qkv_weight,
    out_weight,
    router_weight,
    up_weight,
    down_weight,
    qkv_left,
    qkv_right,
    out_left,
    out_right,
    router_left,
    router_right,
    up_left,
    up_right,
    down_left,
    down_right,
    routes,
    capacity,
    adapter_id,
    cotangent,
):
    images = tokens.shape[0]
    token_count = images * SEQ
    owner_count = lax.axis_size("expert")
    local_experts = up_weight.shape[0]
    experts = owner_count * local_experts
    slots = slot_count(token_count, experts)
    scale = HEAD_DIM ** (-0.5)
    gathered = (
        lax.all_gather(qkv_weight, "shard", axis=0, tiled=True),
        lax.all_gather(out_weight, "shard", axis=0, tiled=True),
        lax.all_gather(router_weight, "shard", axis=0, tiled=True),
        lax.all_gather(qkv_left, "shard", axis=0, tiled=True),
        lax.all_gather(qkv_right, "shard", axis=1, tiled=True),
        lax.all_gather(out_left, "shard", axis=0, tiled=True),
        lax.all_gather(out_right, "shard", axis=0, tiled=True),
        lax.all_gather(router_left, "shard", axis=0, tiled=True),
        lax.all_gather(router_right, "shard", axis=0, tiled=True),
        lax.all_gather(up_weight, "shard", axis=2, tiled=True),
        lax.all_gather(down_weight, "shard", axis=1, tiled=True),
        lax.all_gather(up_left, "shard", axis=1, tiled=True),
        lax.all_gather(up_right, "shard", axis=2, tiled=True),
        lax.all_gather(down_left, "shard", axis=1, tiled=True),
        lax.all_gather(down_right, "shard", axis=2, tiled=True),
    )
    attn_params = tuple(gathered[:9])
    expert_params = tuple(gathered[9:])
    (
        qkv_full,
        out_full,
        router_full,
        qleft_full,
        qright_full,
        oleft_full,
        oright_full,
        rleft_full,
        rright_full,
    ) = attn_params
    rows_in = tokens.reshape(token_count, D).astype(jnp.float32)
    image_hot = (jnp.arange(ADAPTERS, dtype=jnp.int32)[None, :] == adapter_id[:, None]).astype(
        jnp.bfloat16
    )
    token_hot = jnp.repeat(image_hot, SEQ, axis=0)
    token_mask = jnp.repeat(token_hot, RANK, axis=1)
    normed_attn, normal_attn, inverse_attn = layer_norm(rows_in, attn_gain)
    low_attn = normed_attn.astype(jnp.bfloat16)
    qkv_low = (
        product(low_attn, qleft_full).astype(jnp.bfloat16).reshape(token_count, 3, ADAPT_COLS)
        * token_mask[:, None, :]
    )
    qkv_delta = jnp.einsum(
        "tjr,jrd->tjd", qkv_low, qright_full, preferred_element_type=jnp.float32
    ).reshape(token_count, 3 * D)
    qkv_rows = (product(low_attn, qkv_full) + qkv_delta).astype(jnp.bfloat16)
    qkv_split = qkv_rows.reshape(images, SEQ, 3, HEADS, HEAD_DIM)
    queries = qkv_split[:, :, 0]
    key_rows = qkv_split[:, :, 1]
    value_rows = qkv_split[:, :, 2]
    scores = (
        jnp.einsum("bqhd,bkhd->bhqk", queries, key_rows, preferred_element_type=jnp.float32) * scale
    )
    row_max = jnp.max(scores, axis=-1, keepdims=True)
    log_total = row_max + jnp.log(jnp.sum(jnp.exp(scores - row_max), axis=-1, keepdims=True))
    weights_low = jnp.exp(scores - log_total).astype(jnp.bfloat16)
    attended = (
        jnp.einsum("bhqk,bkhd->bqhd", weights_low, value_rows, preferred_element_type=jnp.float32)
        .reshape(token_count, D)
        .astype(jnp.bfloat16)
    )
    out_low = product(attended, oleft_full).astype(jnp.bfloat16) * token_mask
    attn_rows = product(attended, out_full) + product(out_low, oright_full)
    after_attn = rows_in + attn_rows
    normed_moe, normal_moe, inverse_moe = layer_norm(after_attn, moe_gain)
    low_moe = normed_moe.astype(jnp.bfloat16)
    router_low = product(low_moe, rleft_full).astype(jnp.bfloat16) * token_mask
    logits = product(low_moe, router_full) + product(router_low, rright_full)
    router_probs = jax.nn.softmax(logits, axis=-1)
    pair_routes = routes.reshape(token_count, 2).T.reshape(2 * token_count)
    expert_hot = (pair_routes[:, None] == jnp.arange(experts, dtype=jnp.int32)[None, :]).astype(
        jnp.int32
    )
    place = jnp.sum((jnp.cumsum(expert_hot, axis=0) - 1) * expert_hot, axis=1)
    limit = jnp.sum(expert_hot * capacity[None, :], axis=1)
    kept = place < limit
    slot_index = jnp.where(kept, pair_routes * slots + place, experts * slots)
    pair_ids = jnp.arange(2 * token_count, dtype=jnp.int32)
    source = (
        jnp.full((experts * slots + 1,), 2 * token_count, jnp.int32)
        .at[slot_index]
        .set(pair_ids)[: experts * slots]
    )
    token_index = jnp.where(source < 2 * token_count, source % token_count, token_count)
    moe_padded = jnp.concatenate([low_moe, jnp.zeros((1, D), jnp.bfloat16)], axis=0)
    hot_padded = jnp.concatenate([token_hot, jnp.zeros((1, ADAPTERS), jnp.bfloat16)], axis=0)
    sent_rows = moe_padded[token_index].reshape(owner_count, local_experts, slots, D)
    sent_hot = hot_padded[token_index].reshape(owner_count, local_experts, slots, ADAPTERS)
    pair_probs = jnp.concatenate([router_probs, router_probs], axis=0)
    gate = jnp.sum(pair_probs * expert_hot.astype(jnp.float32), axis=1) * kept.astype(jnp.float32)
    grad_out = cotangent.reshape(token_count, D).astype(jnp.float32)
    grad_pairs = jnp.concatenate([grad_out, grad_out], axis=0)
    pair_grad = jnp.concatenate(
        [gate[:, None] * grad_pairs, jnp.zeros((1, D), jnp.float32)], axis=0
    )
    grad_slots = (
        pair_grad[source].astype(jnp.bfloat16).reshape(owner_count, local_experts, slots, D)
    )
    recv_rows, recv_hot = (
        lax.all_to_all(sent_rows, "expert", split_axis=0, concat_axis=0, tiled=True),
        lax.all_to_all(sent_hot, "expert", split_axis=0, concat_axis=0, tiled=True),
    )
    recv_mask = jnp.repeat(recv_hot, RANK, axis=3)
    weight_up, weight_down, left_up, right_up, left_down, right_down = expert_params
    expert_out, expert_saved = expert_forward(
        recv_rows, recv_mask, weight_up, weight_down, left_up, right_up, left_down, right_down
    )
    out_rows = expert_out.astype(jnp.bfloat16)
    back_rows_home = lax.all_to_all(out_rows, "expert", split_axis=0, concat_axis=0, tiled=True)
    home_padded = jnp.concatenate(
        [back_rows_home.reshape(experts * slots, D), jnp.zeros((1, D), jnp.bfloat16)], axis=0
    )
    picked = home_padded[slot_index].astype(jnp.float32)
    weighted = (gate[:, None] * picked).reshape(2, token_count, D)
    final_sum = after_attn + weighted[0] + weighted[1]
    layer_out = final_sum.astype(jnp.bfloat16).reshape(images, SEQ, D)
    gate_grad = jnp.sum(grad_pairs * picked, axis=1) * kept.astype(jnp.float32)
    grad_recv = lax.all_to_all(grad_slots, "expert", split_axis=0, concat_axis=0, tiled=True)
    regathered = (
        lax.all_gather(qkv_weight, "shard", axis=0, tiled=True),
        lax.all_gather(out_weight, "shard", axis=0, tiled=True),
        lax.all_gather(router_weight, "shard", axis=0, tiled=True),
        lax.all_gather(qkv_left, "shard", axis=0, tiled=True),
        lax.all_gather(qkv_right, "shard", axis=1, tiled=True),
        lax.all_gather(out_left, "shard", axis=0, tiled=True),
        lax.all_gather(out_right, "shard", axis=0, tiled=True),
        lax.all_gather(router_left, "shard", axis=0, tiled=True),
        lax.all_gather(router_right, "shard", axis=0, tiled=True),
        lax.all_gather(up_weight, "shard", axis=2, tiled=True),
        lax.all_gather(down_weight, "shard", axis=1, tiled=True),
        lax.all_gather(up_left, "shard", axis=1, tiled=True),
        lax.all_gather(up_right, "shard", axis=2, tiled=True),
        lax.all_gather(down_left, "shard", axis=1, tiled=True),
        lax.all_gather(down_right, "shard", axis=2, tiled=True),
    )
    attn_params = tuple(regathered[:9])
    weight_up, weight_down, left_up, right_up, left_down, right_down = tuple(regathered[9:])
    rows_grad, expert_grads = expert_backward(
        recv_rows,
        recv_mask,
        grad_recv,
        expert_saved,
        weight_up,
        weight_down,
        left_up,
        right_up,
        left_down,
        right_down,
    )
    returned_grad = lax.all_to_all(
        rows_grad.astype(jnp.bfloat16), "expert", split_axis=0, concat_axis=0, tiled=True
    )
    (
        qkv_full,
        out_full,
        router_full,
        qleft_full,
        qright_full,
        oleft_full,
        oright_full,
        rleft_full,
        rright_full,
    ) = attn_params
    grad_padded = jnp.concatenate(
        [returned_grad.reshape(experts * slots, D), jnp.zeros((1, D), jnp.bfloat16)], axis=0
    )
    pair_rows = grad_padded[slot_index].astype(jnp.float32).reshape(2, token_count, D)
    moe_grad = pair_rows[0] + pair_rows[1]
    probs_grad = jnp.sum(
        (gate_grad[:, None] * expert_hot.astype(jnp.float32)).reshape(2, token_count, experts),
        axis=0,
    )
    probs_total = jnp.sum(router_probs * probs_grad, axis=1, keepdims=True)
    logits_grad = (router_probs * (probs_grad - probs_total)).astype(jnp.bfloat16)
    rright_grad = cross_rows(router_low, logits_grad)
    router_grad_low = (back_rows(logits_grad, rright_full) * token_mask).astype(jnp.bfloat16)
    rleft_grad = cross_rows(low_moe, router_grad_low)
    moe_norm_grad = (
        moe_grad + back_rows(logits_grad, router_full) + back_rows(router_grad_low, rleft_full)
    )
    after_grad = grad_out + norm_back(moe_norm_grad, moe_gain, normal_moe, inverse_moe)
    attn_grad = after_grad.astype(jnp.bfloat16)
    oright_grad = cross_rows(out_low, attn_grad)
    out_grad_low = (back_rows(attn_grad, oright_full) * token_mask).astype(jnp.bfloat16)
    oleft_grad = cross_rows(attended, out_grad_low)
    attended_grad = (
        (back_rows(attn_grad, out_full) + back_rows(out_grad_low, oleft_full))
        .astype(jnp.bfloat16)
        .reshape(images, SEQ, HEADS, HEAD_DIM)
    )
    scores_again = (
        jnp.einsum("bqhd,bkhd->bhqk", queries, key_rows, preferred_element_type=jnp.float32) * scale
    )
    weights = jnp.exp(scores_again - log_total)
    weights_again = weights.astype(jnp.bfloat16)
    weights_grad = jnp.einsum(
        "bqhd,bkhd->bhqk", attended_grad, value_rows, preferred_element_type=jnp.float32
    )
    scores_grad = (
        weights * (weights_grad - jnp.sum(weights * weights_grad, axis=-1, keepdims=True))
    ).astype(jnp.bfloat16)
    query_grad = (
        jnp.einsum("bhqk,bkhd->bqhd", scores_grad, key_rows, preferred_element_type=jnp.float32)
        * scale
    )
    key_grad = (
        jnp.einsum("bhqk,bqhd->bkhd", scores_grad, queries, preferred_element_type=jnp.float32)
        * scale
    )
    value_grad = jnp.einsum(
        "bhqk,bqhd->bkhd", weights_again, attended_grad, preferred_element_type=jnp.float32
    )
    qkv_grad = (
        jnp.stack([query_grad, key_grad, value_grad], axis=2)
        .reshape(token_count, 3 * D)
        .astype(jnp.bfloat16)
    )
    qkv_grad_split = qkv_grad.reshape(token_count, 3, D)
    qright_grad = jnp.einsum(
        "tjr,tjd->jrd", qkv_low, qkv_grad_split, preferred_element_type=jnp.float32
    )
    qkv_grad_low = (
        (
            jnp.einsum(
                "tjd,jrd->tjr", qkv_grad_split, qright_full, preferred_element_type=jnp.float32
            )
            * token_mask[:, None, :]
        )
        .astype(jnp.bfloat16)
        .reshape(token_count, 3 * ADAPT_COLS)
    )
    qleft_grad = cross_rows(low_attn, qkv_grad_low)
    attn_norm_grad = back_rows(qkv_grad, qkv_full) + back_rows(qkv_grad_low, qleft_full)
    tokens_grad = (
        after_grad + norm_back(attn_norm_grad, attn_gain, normal_attn, inverse_attn)
    ).reshape(images, SEQ, D)
    uleft_part, uright_part, dleft_part, dright_part = expert_grads
    summed = (
        lax.psum_scatter(
            qleft_grad.astype(jnp.bfloat16), "shard", scatter_dimension=0, tiled=True
        ).astype(jnp.float32),
        lax.psum_scatter(
            qright_grad.astype(jnp.bfloat16), "shard", scatter_dimension=1, tiled=True
        ).astype(jnp.float32),
        lax.psum_scatter(
            oleft_grad.astype(jnp.bfloat16), "shard", scatter_dimension=0, tiled=True
        ).astype(jnp.float32),
        lax.psum_scatter(
            oright_grad.astype(jnp.bfloat16), "shard", scatter_dimension=0, tiled=True
        ).astype(jnp.float32),
        lax.psum_scatter(
            rleft_grad.astype(jnp.bfloat16), "shard", scatter_dimension=0, tiled=True
        ).astype(jnp.float32),
        lax.psum_scatter(
            rright_grad.astype(jnp.bfloat16), "shard", scatter_dimension=0, tiled=True
        ).astype(jnp.float32),
        lax.psum_scatter(
            uleft_part.astype(jnp.bfloat16), "shard", scatter_dimension=1, tiled=True
        ).astype(jnp.float32),
        lax.psum_scatter(
            uright_part.astype(jnp.bfloat16), "shard", scatter_dimension=2, tiled=True
        ).astype(jnp.float32),
        lax.psum_scatter(
            dleft_part.astype(jnp.bfloat16), "shard", scatter_dimension=1, tiled=True
        ).astype(jnp.float32),
        lax.psum_scatter(
            dright_part.astype(jnp.bfloat16), "shard", scatter_dimension=2, tiled=True
        ).astype(jnp.float32),
    )
    uleft_grad, uright_grad, dleft_grad, dright_grad = tuple(summed[6:])
    qleft_sum, qright_sum, oleft_sum, oright_sum, rleft_sum, rright_sum = (
        lax.psum(summed[0].astype(jnp.bfloat16), "expert").astype(jnp.float32),
        lax.psum(summed[1].astype(jnp.bfloat16), "expert").astype(jnp.float32),
        lax.psum(summed[2].astype(jnp.bfloat16), "expert").astype(jnp.float32),
        lax.psum(summed[3].astype(jnp.bfloat16), "expert").astype(jnp.float32),
        lax.psum(summed[4].astype(jnp.bfloat16), "expert").astype(jnp.float32),
        lax.psum(summed[5].astype(jnp.bfloat16), "expert").astype(jnp.float32),
    )
    return (
        layer_out,
        tokens_grad,
        qleft_sum,
        qright_sum,
        oleft_sum,
        oright_sum,
        rleft_sum,
        rright_sum,
        uleft_grad,
        uright_grad,
        dleft_grad,
        dright_grad,
    )


PLANES, COLS_X, ROWS_Y, CORES = 4, 2, 2, 2
SEQ_PAD = 208
WIDE = 1536
FF_PART = 512
W_ROWS = 704
G_ROWS = 320
QUAD = 4 * HEAD_DIM
BF16 = jnp.bfloat16
F32 = jnp.float32


def pairs_of(move):
    pairs = []
    for z in range(PLANES):
        for x in range(COLS_X):
            for y in range(ROWS_Y):
                for c in range(CORES):
                    nz, nx, ny, nc = move(z, x, y, c)
                    source = (z * COLS_X + x) * ROWS_Y * CORES + y * CORES + c
                    target = (nz * COLS_X + nx) * ROWS_Y * CORES + ny * CORES + nc
                    pairs.append((source, target))
    return pairs


OVER_X = pairs_of(lambda z, x, y, c: (z, 1 - x, y, c))
OVER_Y = pairs_of(lambda z, x, y, c: (z, x, 1 - y, c))
OVER_CORE = pairs_of(lambda z, x, y, c: (z, x, y, 1 - c))


def from_plane(ahead):
    return pairs_of(lambda z, x, y, c: ((z - ahead) % PLANES, x, y, c))


def to_plane(ahead):
    return pairs_of(lambda z, x, y, c: ((z + ahead) % PLANES, x, y, c))


def move(value, pairs):
    return lax.ppermute(value, ("expert", "shard"), pairs)


def dot(left, right):
    return jnp.dot(left, right, preferred_element_type=F32)


def dot_bt(left, right):
    return lax.dot_general(left, right, (((1,), (1,)), ((), ())), preferred_element_type=F32)


def dot_at(left, right):
    return lax.dot_general(left, right, (((0,), (0,)), ((), ())), preferred_element_type=F32)


def normal_of(values):
    centred = values - jnp.mean(values, axis=-1, keepdims=True)
    inverse = lax.rsqrt(jnp.mean(centred * centred, axis=-1, keepdims=True) + EPSILON)
    return (centred * inverse, inverse)


C_QKV, C_QL, C_OUT, C_OL, C_RL, C_RW = 0, 1536, 1920, 2432, 2560, 2688
LEFT_COLS = 2816
R_OUT, R_ROUTER = 1536, 2048
RIGHT_COLS = 2176


def load_weights(place_ref, left_refs, right_refs, left_all, right_all, sems):
    copies = []
    own = place_ref[0]
    for k in range(4):
        quarter = own ^ ((k % 2) * 2 + k // 2)
        rows = pl.ds(pl.multiple_of(quarter * 128, 128), 128)
        copies.append(pltpu.make_async_copy(left_refs[k], left_all.at[rows], sems.at[2 * k]))
        rows = pl.ds(pl.multiple_of(quarter * 32, 32), 32)
        copies.append(pltpu.make_async_copy(right_refs[k], right_all.at[rows], sems.at[2 * k + 1]))
    for copy in copies:
        copy.start()
    for copy in copies:
        copy.wait()


def image_mask(adapter, cols):
    lane = lax.broadcasted_iota(jnp.int32, (1, cols), 1)
    return ((lane % ADAPT_COLS) // RANK == adapter).astype(F32)


def head_lanes(rows):
    return lax.broadcasted_iota(jnp.int32, (rows, QUAD), 1) // HEAD_DIM


def stack_heads(quad):
    lanes = head_lanes(quad.shape[0])
    zero = jnp.zeros_like(quad)
    return jnp.concatenate([jnp.where(lanes == h, quad, zero) for h in range(4)], axis=0)


def unstack_heads(stacked):
    rows = stacked.shape[0] // 4
    lanes = head_lanes(rows)
    total = jnp.where(lanes == 0, stacked[:rows], 0.0)
    for h in range(1, 4):
        total = jnp.where(lanes == h, stacked[h * rows : (h + 1) * rows], total)
    return total


def attn_forward_kernel(
    place_ref,
    ids_ref,
    tokens_ref,
    cot_ref,
    again_ref,
    mgain_ref,
    l0,
    l1,
    l2,
    l3,
    r0,
    r1,
    r2,
    r3,
    wide_ref,
    after_ref,
    probs_ref,
    qkv_ref,
    weights_ref,
    att_ref,
    lows_ref,
    left_all,
    right_all,
    sems,
):
    step = pl.program_id(0)

    @pl.when(step == 0)
    def _():
        load_weights(place_ref, (l0, l1, l2, l3), (r0, r1, r2, r3), left_all, right_all, sems)

    adapter = ids_ref[step]
    live = lax.broadcasted_iota(jnp.int32, (SEQ_PAD, 1), 0) < SEQ
    rows_in = jnp.where(live, tokens_ref[0].astype(F32), 0.0)
    cot = jnp.where(live, cot_ref[0].astype(F32), 0.0).astype(BF16)
    normal, _ = normal_of(rows_in)
    low_attn = (normal * again_ref[...]).astype(BF16)
    mask = image_mask(adapter, 3 * ADAPT_COLS)
    qkv_low = dot(low_attn, left_all[:, C_QL:C_OUT]).astype(BF16) * mask.astype(BF16)
    lows_ref[0, :, 0:384] = qkv_low
    for j in range(3):
        cols = slice(j * D, (j + 1) * D)
        part = dot(low_attn, left_all[:, cols]) + dot(
            qkv_low[:, j * ADAPT_COLS : (j + 1) * ADAPT_COLS], right_all[:, cols]
        )
        qkv_ref[0, :, cols] = part.astype(BF16)
    key_live = lax.broadcasted_iota(jnp.int32, (1, SEQ_PAD), 1) < SEQ
    for quad in range(HEADS // 4):
        at = quad * QUAD
        queries = stack_heads(qkv_ref[0, :, at : at + QUAD])
        keys = qkv_ref[0, :, D + at : D + at + QUAD]
        values = qkv_ref[0, :, 2 * D + at : 2 * D + at + QUAD]
        scores = jnp.where(key_live, dot_bt(queries, keys) * (HEAD_DIM**-0.5), -1e30)
        powers = jnp.exp(scores - jnp.max(scores, axis=-1, keepdims=True))
        weights = powers * (1.0 / jnp.sum(powers, axis=-1, keepdims=True))
        weights = weights.astype(BF16)
        weights_ref[0, quad] = weights
        att_ref[0, :, at : at + QUAD] = unstack_heads(dot(weights, values)).astype(BF16)
    attended = att_ref[0]
    small_mask = mask[:, :ADAPT_COLS]
    out_low = dot(attended, left_all[:, C_OL:C_RL]).astype(BF16) * small_mask.astype(BF16)
    after = (
        rows_in
        + dot(attended, left_all[:, C_OUT:C_OL])
        + dot(out_low, right_all[:, R_OUT:R_ROUTER])
    )
    after_ref[0] = after
    normal, _ = normal_of(after)
    low_moe = (normal * mgain_ref[...]).astype(BF16)
    router_low = dot(low_moe, left_all[:, C_RL:C_RW]).astype(BF16) * small_mask.astype(BF16)
    lows_ref[0, :, 384:512] = out_low
    lows_ref[0, :, 512:640] = router_low
    logits = dot(low_moe, left_all[:, C_RW:]) + dot(router_low, right_all[:, R_ROUTER:])
    lane = lax.broadcasted_iota(jnp.int32, (1, 128), 1)
    logits = jnp.where(lane < PLANES * COLS_X, logits, -1e30)
    powers = jnp.exp(logits - jnp.max(logits, axis=-1, keepdims=True))
    probs = powers / jnp.sum(powers, axis=-1, keepdims=True)
    probs_ref[0] = probs
    high = probs.astype(BF16)
    middle = (probs - high.astype(F32)).astype(BF16)
    lowest = (probs - high.astype(F32) - middle.astype(F32)).astype(BF16)
    wide_ref[0, :, 0:512] = low_moe
    wide_ref[0, :, 512:1024] = cot
    wide_ref[0, :, 1024:1152] = jnp.broadcast_to(small_mask, (SEQ_PAD, 128)).astype(BF16)
    wide_ref[0, :, 1152:1280] = high
    wide_ref[0, :, 1280:1408] = middle
    wide_ref[0, :, 1408:1536] = lowest


def whole(shape):
    return pl.BlockSpec(shape, lambda *_: (0,) * len(shape))


def per_image(*shape):
    return pl.BlockSpec((1,) + shape, lambda i: (i,) + (0,) * len(shape))


ANYWHERE = pl.BlockSpec(memory_space=pl.ANY)
SCALARS = pl.BlockSpec(memory_space=pltpu.SMEM)


def attn_forward(place, ids, tokens, cot, again, mgain, lefts, rights):
    images = tokens.shape[0]
    out = lambda cols, dtype: jax.ShapeDtypeStruct((images, SEQ_PAD, cols), dtype)
    return pl.pallas_call(
        attn_forward_kernel,
        grid=(images,),
        in_specs=[SCALARS, SCALARS, per_image(SEQ_PAD, D), per_image(SEQ_PAD, D)]
        + [whole((1, D))] * 2
        + [ANYWHERE] * 8,
        out_specs=[
            per_image(SEQ_PAD, WIDE),
            per_image(SEQ_PAD, D),
            per_image(SEQ_PAD, 128),
            per_image(SEQ_PAD, 3 * D),
            per_image(2, 4 * SEQ_PAD, SEQ_PAD),
            per_image(SEQ_PAD, D),
            per_image(SEQ_PAD, 640),
        ],
        out_shape=[
            out(WIDE, BF16),
            out(D, F32),
            out(128, F32),
            out(3 * D, BF16),
            jax.ShapeDtypeStruct((images, 2, 4 * SEQ_PAD, SEQ_PAD), BF16),
            out(D, BF16),
            out(640, BF16),
        ],
        scratch_shapes=[
            pltpu.VMEM((D, LEFT_COLS), BF16),
            pltpu.VMEM((ADAPT_COLS, RIGHT_COLS), BF16),
            pltpu.SemaphoreType.DMA((8,)),
        ],
        compiler_params=pltpu.CompilerParams(vmem_limit_bytes=58 * 2**20),
        cost_estimate=pl.CostEstimate(flops=6 * 10**9, bytes_accessed=20 * 10**6, transcendentals=10**6),
        name="attn_forward",
    )(place, ids, tokens, cot, again, mgain, *lefts, *rights)


def route_kernel(cols_ref, rows_ref, cap_ref, capt_ref, slot_ref, slott_ref):
    count = cols_ref.shape[1]
    lane = lax.broadcasted_iota(jnp.int32, (count, 128), 1)
    first = lane == cols_ref[0, :, 0:1]
    second = lane == cols_ref[0, :, 1:2]
    here = lax.broadcasted_iota(jnp.int32, (count, count), 0)
    there = lax.broadcasted_iota(jnp.int32, (count, count), 1)
    below = (there < here).astype(F32).astype(BF16)
    hot0, hot1 = first.astype(F32), second.astype(F32)
    place0 = dot(below, hot0.astype(BF16))
    place1 = dot(below, hot1.astype(BF16)) + jnp.sum(hot0, axis=0, keepdims=True)
    slot = jnp.where(first, place0, jnp.where(second, place1, 1e6))
    slot_ref[0] = jnp.where(slot < cap_ref[...], slot, -1.0)
    expert = lax.broadcasted_iota(jnp.int32, (8, count), 0)
    first = expert == rows_ref[0, 0:1, :]
    second = expert == rows_ref[0, 1:2, :]
    above = (here < there).astype(F32).astype(BF16)
    hot0, hot1 = first.astype(F32), second.astype(F32)
    place0 = dot(hot0.astype(BF16), above)
    place1 = dot(hot1.astype(BF16), above) + jnp.sum(hot0, axis=1, keepdims=True)
    slot = jnp.where(first, place0, jnp.where(second, place1, 1e6))
    slott_ref[0] = jnp.where(slot < capt_ref[...], slot, -1.0)


def route_slots(cols, rows, cap, capt):
    groups, count, _ = cols.shape
    return pl.pallas_call(
        route_kernel,
        grid=(groups,),
        in_specs=[per_image(count, 2), per_image(2, count), whole((1, 128)), whole((8, 1))],
        out_specs=[per_image(count, 128), per_image(8, count)],
        out_shape=[
            jax.ShapeDtypeStruct((groups, count, 128), F32),
            jax.ShapeDtypeStruct((groups, 8, count), F32),
        ],
        compiler_params=pltpu.CompilerParams(vmem_limit_bytes=40 * 2**20),
        cost_estimate=pl.CostEstimate(flops=10**9, bytes_accessed=3 * 10**6, transcendentals=0),
        name="route_slots",
    )(cols, rows, cap, capt)


def gelu_parts(v):
    bell = jnp.exp(-0.5 * (v * v))
    t = 1.0 / (1.0 + (0.3275911 * 0.7071067811865476) * jnp.abs(v))
    poly = t * (0.254829592 + t * (-0.284496736 + t * (1.421413741 + t * (-1.453152027 + t * 1.061405429))))
    tail = (0.5 * poly) * bell
    cdf = jnp.where(v >= 0, 1.0 - tail, tail)
    return (cdf, cdf + v * (bell * 0.3989422804014327))


def experts_kernel(
    slots,
    ids_ref,
    wide0,
    wide1,
    slot_ref,
    slott_ref,
    old_sum,
    old_grad,
    old_probs,
    *rest,
):
    packs, (sum_ref, grad_ref, probs_ref, g_ref, gs_ref) = rest[:8], rest[8:13]
    (held, rows, grads, masks, out_acc, back_acc, low, dgrad, dlow_acc, ugrad_acc, hidden, pre_grad, left_up, right_down, wide_out, sems) = rest[13:]
    copies = [pltpu.make_async_copy(packs[k], held.at[k], sems.at[k]) for k in range(8)]
    for copy in copies:
        copy.start()
    wides = (wide0, wide1)
    count = wide0.shape[0]
    total = 2 * slots
    chunk = 128
    sum_ref[...] = old_sum[...]
    grad_ref[...] = old_grad[...]
    probs_ref[...] = old_probs[...]
    for copy in copies:
        copy.wait()

    @pl.loop(0, 2)
    def _(xr):
        expert = ids_ref[xr]
        lane = lax.broadcasted_iota(jnp.int32, (1, 128), 1)
        chosen = (lane == expert).astype(F32)
        for g in range(2):
            at = slice(g * slots, (g + 1) * slots)
            number = lax.broadcasted_iota(jnp.int32, (slots, count), 0).astype(F32)
            hot = (slott_ref[g, pl.ds(expert, 1), :] == number).astype(F32).astype(BF16)
            rows[at, :] = dot(hot, wides[g][:, 0:512]).astype(BF16)
            rest_cols = dot(hot, wides[g][:, 1024:1536])
            masks[at, :] = rest_cols[:, 0:128]
            gates = rest_cols[:, 128:256] + rest_cols[:, 256:384] + rest_cols[:, 384:512]
            gate = jnp.sum(gates * chosen, axis=1, keepdims=True)
            grads[at, :] = (gate * dot(hot, wides[g][:, 512:1024])).astype(BF16)
        for yr in range(2):
            for cr in range(2):
                quarter = ids_ref[2 + 2 * yr + cr]
                cols = pl.ds(pl.multiple_of(quarter * 128, 128), 128)
                for i in range(4):
                    block = held[4 * xr + 2 * yr, 640 + 32 * cr : 672 + 32 * cr, 128 * i : 128 * (i + 1)]
                    left_up[pl.ds(pl.multiple_of(quarter * 128 + 32 * i, 32), 32), :] = block
                    block = held[4 * xr + 2 * yr + 1, 640 + 32 * cr : 672 + 32 * cr, 128 * i : 128 * (i + 1)]
                    right_down[32 * i : 32 * (i + 1), cols] = block
        low[...] = (dot(rows[...], left_up[...]).astype(BF16).astype(F32) * masks[...]).astype(BF16)
        dgrad[...] = (dot_bt(grads[...], right_down[...]) * masks[...]).astype(BF16)
        low_t = low[...].T
        dgrad_t = dgrad[...].T
        out_acc[...] = jnp.zeros_like(out_acc)
        back_acc[...] = jnp.zeros_like(back_acc)
        dlow_acc[...] = jnp.zeros_like(dlow_acc)
        ugrad_acc[...] = jnp.zeros_like(ugrad_acc)
        for yr in range(2):
            ka, kb = 4 * xr + 2 * yr, 4 * xr + 2 * yr + 1

            @pl.loop(0, total // chunk)
            def _(m):
                at = pl.ds(pl.multiple_of(m * chunk, chunk), chunk)
                x, d = rows[at, :], grads[at, :]
                lo, dg = low[at, :], dgrad[at, :]
                for n in range(2):
                    cols = slice(n * 256, (n + 1) * 256)
                    pre = dot(x, held[ka, 0:512, cols]) + dot(lo, held[ka, 512:640, cols])
                    cdf, slope = gelu_parts(pre)
                    hidden[at, cols] = (pre * cdf).astype(BF16)
                    back = dot_bt(d, held[kb, cols, :])
                    for i in range(2):
                        b = 2 * n + i
                        part = back[:, i * 128 : (i + 1) * 128] + dot_bt(dg, held[kb, 512:640, b * 128 : (b + 1) * 128])
                        pre_grad[at, b * 128 : (b + 1) * 128] = (part * slope[:, i * 128 : (i + 1) * 128]).astype(BF16)
                h, p = hidden[at, :], pre_grad[at, :]
                out_acc[at, :] += dot(h, held[kb, 0:512, :])
                back_acc[at, :] += dot_bt(p, held[ka, 0:512, :])
                ugrad_acc[at, :] += dot_bt(p, held[ka, 512:640, :])
                part = dot(h[:, 0:128], held[kb, 512:640, 0:128])
                for i in range(1, 4):
                    part += dot(h[:, i * 128 : (i + 1) * 128], held[kb, 512:640, i * 128 : (i + 1) * 128])
                dlow_acc[at, :] += part

            g_ref[xr, yr, 0:128, :] = dot(dgrad_t, hidden[...]).astype(BF16)
            g_ref[xr, yr, 128:256, :] = dot(low_t, pre_grad[...]).astype(BF16)
        dlow = (dlow_acc[...] * masks[...]).astype(BF16)
        ugrad = (ugrad_acc[...] * masks[...]).astype(BF16)
        wide_out[:, 0:512] = (out_acc[...] + dot(dlow, right_down[...])).astype(BF16)
        wide_out[:, 512:1024] = (back_acc[...] + dot_bt(ugrad, left_up[...])).astype(BF16)
        out_acc[0:128, :] = dot(ugrad.T, rows[...])
        out_acc[128:256, :] = dot(dlow.T, grads[...])
        for yr in range(2):
            for cr in range(2):
                quarter = ids_ref[2 + 2 * yr + cr]
                cols = pl.ds(pl.multiple_of(quarter * 128, 128), 128)
                for k in range(2):
                    block = out_acc[128 * k : 128 * (k + 1), cols].astype(BF16)
                    for i in range(4):
                        piece = block[32 * i : 32 * (i + 1), :]
                        where = slice(128 * i, 128 * (i + 1))
                        if cr == 0:
                            g_ref[xr, yr, 256 + 32 * k : 288 + 32 * k, where] = piece
                        else:
                            gs_ref[xr, yr, 32 * k : 32 * (k + 1), where] = piece
        for g in range(2):
            at = slice(g * slots, (g + 1) * slots)
            mine = jnp.sum(slot_ref[g] * chosen, axis=1, keepdims=True)
            gates = (
                wides[g][:, 1152:1280].astype(F32)
                + wides[g][:, 1280:1408].astype(F32)
                + wides[g][:, 1408:1536].astype(F32)
            )
            gate = jnp.sum(gates * chosen, axis=1, keepdims=True)
            number = lax.broadcasted_iota(jnp.int32, (count, slots), 1).astype(F32)
            hot = (mine == number).astype(F32).astype(BF16)
            grad_ref[g] += dot(hot, wide_out[at, 512:1024])
            picked = dot(hot, wide_out[at, 0:512])
            sum_ref[g] += gate * picked
            inner = jnp.sum(picked * wides[g][:, 512:1024].astype(F32), axis=1, keepdims=True)
            probs_ref[g] += inner * chosen


def experts(ids, wide0, wide1, slot, slott, old, packs, slots):
    count = wide0.shape[0]
    total = 2 * slots
    sums = jax.ShapeDtypeStruct((2, count, D), F32)
    probs = jax.ShapeDtypeStruct((2, count, 128), F32)
    vmem = pl.BlockSpec(memory_space=pltpu.VMEM)
    return pl.pallas_call(
        functools.partial(experts_kernel, slots),
        in_specs=[SCALARS] + [vmem] * 7 + [ANYWHERE] * 8,
        out_specs=[vmem] * 5,
        out_shape=[
            sums,
            sums,
            probs,
            jax.ShapeDtypeStruct((2, 2, G_ROWS, 512), BF16),
            jax.ShapeDtypeStruct((2, 2, 64, 512), BF16),
        ],
        scratch_shapes=[
            pltpu.VMEM((8, W_ROWS, 512), BF16),
            pltpu.VMEM((total, D), BF16),
            pltpu.VMEM((total, D), BF16),
            pltpu.VMEM((total, 128), F32),
            pltpu.VMEM((total, D), F32),
            pltpu.VMEM((total, D), F32),
            pltpu.VMEM((total, 128), BF16),
            pltpu.VMEM((total, 128), BF16),
            pltpu.VMEM((total, 128), F32),
            pltpu.VMEM((total, 128), F32),
            pltpu.VMEM((total, FF_PART), BF16),
            pltpu.VMEM((total, FF_PART), BF16),
            pltpu.VMEM((D, 128), BF16),
            pltpu.VMEM((128, D), BF16),
            pltpu.VMEM((total, 2 * D), BF16),
            pltpu.SemaphoreType.DMA((8,)),
        ],
        compiler_params=pltpu.CompilerParams(vmem_limit_bytes=61 * 2**20),
        cost_estimate=pl.CostEstimate(flops=14 * 10**9, bytes_accessed=30 * 10**6, transcendentals=4 * 10**6),
        name="experts",
    )(ids, wide0, wide1, slot, slott, *old, *packs)


def attn_backward_kernel(
    place_ref,
    ids_ref,
    tokens_ref,
    cot_ref,
    again_ref,
    mgain_ref,
    after_ref,
    probs_ref,
    qkv_ref,
    weights_ref,
    att_ref,
    lows_ref,
    low_moe_ref,
    sum_ref,
    grad_ref,
    pgrad_ref,
    sum2_ref,
    grad2_ref,
    pgrad2_ref,
    l0,
    l1,
    l2,
    l3,
    r0,
    r1,
    r2,
    r3,
    out_ref,
    tgrad_ref,
    lefts_ref,
    rights_ref,
    rright_ref,
    left_all,
    right_all,
    qgrad,
    sems,
):
    step = pl.program_id(0)

    @pl.when(step == 0)
    def _():
        load_weights(place_ref, (l0, l1, l2, l3), (r0, r1, r2, r3), left_all, right_all, sems)
        lefts_ref[...] = jnp.zeros_like(lefts_ref)
        rights_ref[...] = jnp.zeros_like(rights_ref)
        rright_ref[...] = jnp.zeros_like(rright_ref)

    adapter = ids_ref[step]
    live = lax.broadcasted_iota(jnp.int32, (SEQ_PAD, 1), 0) < SEQ
    mask = image_mask(adapter, 3 * ADAPT_COLS)
    small_mask = mask[:, :ADAPT_COLS]
    after = after_ref[0]
    out_ref[0] = (after + sum_ref[0] + sum2_ref[0, 0].astype(F32)).astype(BF16)
    cot = jnp.where(live, cot_ref[0].astype(F32), 0.0)
    probs = probs_ref[0]
    pgrad = pgrad_ref[0] + pgrad2_ref[0]
    lgrad = (probs * (pgrad - jnp.sum(probs * pgrad, axis=-1, keepdims=True))).astype(BF16)
    out_low = lows_ref[0, :, 384:512]
    router_low = lows_ref[0, :, 512:640]
    rright_ref[...] += dot_at(router_low, lgrad)
    rglow = (dot_bt(lgrad, right_all[:, R_ROUTER:]) * small_mask).astype(BF16)
    lefts_ref[512:640, :] += dot_at(rglow, low_moe_ref[0])
    mgrad = (
        grad_ref[0]
        + grad2_ref[0, 0].astype(F32)
        + dot_bt(lgrad, left_all[:, C_RW:])
        + dot_bt(rglow, left_all[:, C_RL:C_RW])
    )
    normal, inverse = normal_of(after)
    after_grad = cot + norm_back(mgrad, mgain_ref[...], normal, inverse)
    agrad = after_grad.astype(BF16)
    rights_ref[384:512, :] += dot_at(out_low, agrad)
    oglow = (dot_bt(agrad, right_all[:, R_OUT:R_ROUTER]) * small_mask).astype(BF16)
    lefts_ref[384:512, :] += dot_at(oglow, att_ref[0])
    att_grad = (dot_bt(agrad, left_all[:, C_OUT:C_OL]) + dot_bt(oglow, left_all[:, C_OL:C_RL])).astype(BF16)
    scale = HEAD_DIM**-0.5
    for quad in range(HEADS // 4):
        at = quad * QUAD
        queries = stack_heads(qkv_ref[0, :, at : at + QUAD])
        keys = qkv_ref[0, :, D + at : D + at + QUAD]
        values = qkv_ref[0, :, 2 * D + at : 2 * D + at + QUAD]
        weights = weights_ref[0, quad]
        grad_out = stack_heads(att_grad[:, at : at + QUAD])
        wide = weights.astype(F32)
        wgrad = dot_bt(grad_out, values)
        sgrad = (wide * (wgrad - jnp.sum(wide * wgrad, axis=-1, keepdims=True))).astype(BF16)
        qgrad[:, at : at + QUAD] = (unstack_heads(dot(sgrad, keys)) * scale).astype(BF16)
        qgrad[:, D + at : D + at + QUAD] = (dot_at(sgrad, queries) * scale).astype(BF16)
        qgrad[:, 2 * D + at : 2 * D + at + QUAD] = dot_at(weights, grad_out).astype(BF16)
    rows_in = jnp.where(live, tokens_ref[0].astype(F32), 0.0)
    normal, inverse = normal_of(rows_in)
    low_attn = (normal * again_ref[...]).astype(BF16)
    ngrad = dot_bt(qgrad[...], left_all[:, 0 : 3 * D])
    for j in range(3):
        part = qgrad[:, j * D : (j + 1) * D]
        cols = slice(j * 128, (j + 1) * 128)
        rights_ref[cols, :] += dot_at(lows_ref[0, :, cols], part)
        qglow = (dot_bt(part, right_all[:, j * D : (j + 1) * D]) * small_mask).astype(BF16)
        lefts_ref[cols, :] += dot_at(qglow, low_attn)
        ngrad += dot_bt(qglow, left_all[:, C_QL + j * 128 : C_QL + (j + 1) * 128])
    tgrad_ref[0] = after_grad + norm_back(ngrad, again_ref[...], normal, inverse)


def attn_backward(place, ids, tokens, cot, again, mgain, kept, own, other, lefts, rights):
    images = tokens.shape[0]
    after, probs, qkv, weights, att, lows, wide = kept
    vec = whole((1, D))
    pair = lambda k: pl.BlockSpec((1, 1, SEQ_PAD, D), lambda i: (k, i, 0, 0))
    return pl.pallas_call(
        attn_backward_kernel,
        grid=(images,),
        in_specs=[SCALARS, SCALARS, per_image(SEQ_PAD, D), per_image(SEQ_PAD, D), vec, vec]
        + [
            per_image(SEQ_PAD, D),
            per_image(SEQ_PAD, 128),
            per_image(SEQ_PAD, 3 * D),
            per_image(2, 4 * SEQ_PAD, SEQ_PAD),
            per_image(SEQ_PAD, D),
            per_image(SEQ_PAD, 640),
            per_image(SEQ_PAD, D),
            per_image(SEQ_PAD, D),
            per_image(SEQ_PAD, D),
            per_image(SEQ_PAD, 128),
            pair(0),
            pair(1),
            per_image(SEQ_PAD, 128),
        ]
        + [ANYWHERE] * 8,
        out_specs=[
            per_image(SEQ_PAD, D),
            per_image(SEQ_PAD, D),
            whole((640, D)),
            whole((512, D)),
            whole((128, 128)),
        ],
        out_shape=[
            jax.ShapeDtypeStruct((images, SEQ, D), BF16),
            jax.ShapeDtypeStruct((images, SEQ, D), F32),
            jax.ShapeDtypeStruct((640, D), F32),
            jax.ShapeDtypeStruct((512, D), F32),
            jax.ShapeDtypeStruct((128, 128), F32),
        ],
        scratch_shapes=[
            pltpu.VMEM((D, LEFT_COLS), BF16),
            pltpu.VMEM((ADAPT_COLS, RIGHT_COLS), BF16),
            pltpu.VMEM((SEQ_PAD, 3 * D), BF16),
            pltpu.SemaphoreType.DMA((8,)),
        ],
        compiler_params=pltpu.CompilerParams(vmem_limit_bytes=60 * 2**20),
        cost_estimate=pl.CostEstimate(flops=8 * 10**9, bytes_accessed=30 * 10**6, transcendentals=10**5),
        name="attn_backward",
    )(
        place, ids, tokens, cot, again, mgain, after, probs, qkv, weights, att, lows, wide,
        *own, *other, *lefts, *rights,
    )


def plane_gather(pack_a, pack_b):
    xa, yb = move(pack_a, OVER_X), move(pack_b, OVER_Y)
    ya, xb = move(pack_a, OVER_Y), move(pack_b, OVER_X)
    da, db = move(xa, OVER_Y), move(yb, OVER_X)
    return (pack_a, pack_b, ya, yb, xa, xb, da, db)


def side_by_side(block):
    rows, cols = block.shape
    return block.reshape(4, rows // 4, cols).transpose(1, 0, 2).reshape(rows // 4, 4 * cols)


def stacked_again(block):
    rows, cols = block.shape
    return block.reshape(rows, 4, cols // 4).transpose(1, 0, 2).reshape(rows * 4, cols // 4)


def gathered_path(
    tokens,
    attn_gain,
    moe_gain,
    qkv_weight,
    out_weight,
    router_weight,
    up_weight,
    down_weight,
    qkv_left,
    qkv_right,
    out_left,
    out_right,
    router_left,
    router_right,
    up_left,
    up_right,
    down_left,
    down_right,
    routes,
    capacity,
    adapter_id,
    cotangent,
):
    images = tokens.shape[0]
    count = images * SEQ_PAD
    slots = (slot_count(images * SEQ, PLANES * COLS_X) + 15) // 16 * 16
    owner, shard = lax.axis_index("expert"), lax.axis_index("shard")
    plane, col = owner // COLS_X, owner % COLS_X
    row, core = shard // CORES, shard % CORES
    place = shard.reshape(1).astype(jnp.int32)

    pad8 = lambda w: jnp.pad(w, ((0, 0), (0, 120)))
    left = jnp.concatenate(
        [qkv_weight, qkv_left, out_weight, out_left, router_left, pad8(router_weight)], axis=1
    )
    right = jnp.concatenate(
        [qkv_right[0], qkv_right[1], qkv_right[2], out_right, pad8(router_right)], axis=1
    )
    left_y, right_y = move(left, OVER_Y), move(right, OVER_Y)
    left_c, right_c = move(left, OVER_CORE), move(right, OVER_CORE)
    lefts = (left, left_y, left_c, move(left_y, OVER_CORE))
    rights = (right, right_y, right_c, move(right_y, OVER_CORE))

    small_a, small_b = side_by_side(up_left[0]), side_by_side(down_right[0])
    pack_a = jnp.concatenate([up_weight[0], up_right[0], small_a, move(small_a, OVER_CORE)], axis=0)
    pack_b = jnp.concatenate(
        [down_weight[0], side_by_side(down_left[0]), small_b, move(small_b, OVER_CORE)], axis=0
    )
    packs = []
    for ahead in range(PLANES):
        pairs = from_plane(ahead)
        a, b = (pack_a, pack_b) if ahead == 0 else (move(pack_a, pairs), move(pack_b, pairs))
        packs.append(plane_gather(a, b))

    mine = jnp.pad(routes, ((0, 0), (0, SEQ_PAD - SEQ), (0, 0)), constant_values=-1).reshape(count, 2)
    cols = jnp.stack([mine, move(mine, OVER_CORE)])
    rows = cols.transpose(0, 2, 1)
    limit = capacity.astype(F32)
    slot, slott = route_slots(
        cols, rows, jnp.pad(limit, (0, 128 - limit.shape[0])).reshape(1, 128), limit.reshape(-1, 1)
    )

    again, mgain = attn_gain.reshape(1, D), moe_gain.reshape(1, D)
    wide, after, probs, qkv, weights, att, lows = attn_forward(
        place, adapter_id, tokens, cotangent, again, mgain, lefts, rights
    )
    wide_own = wide.reshape(count, WIDE)
    wide_other = move(wide_own, OVER_CORE)
    done = (
        jnp.zeros((2, count, D), F32),
        jnp.zeros((2, count, D), F32),
        jnp.zeros((2, count, 128), F32),
    )
    grads, sides = [], []
    quarters = [((row + yr) % 2) * 2 + (core + cr) % 2 for yr in range(2) for cr in range(2)]
    for ahead in range(PLANES):
        at = (plane + ahead) % PLANES * COLS_X
        ids = jnp.stack([at + col, at + 1 - col] + quarters).astype(jnp.int32)
        *done, grad, side = experts(ids, wide_own, wide_other, slot, slott, done, packs[ahead], slots)
        grads.append(grad)
        sides.append(side)
    sums, backs, pgrads = done
    shape4 = (images, SEQ_PAD, D)
    sent = jnp.stack([sums[1], backs[1]]).astype(BF16).reshape((2,) + shape4)
    other = move(sent, OVER_CORE)
    other_p = move(pgrads[1], OVER_CORE).reshape(images, SEQ_PAD, 128)
    layer_out, tokens_grad, lgrad, rgrad, rright = attn_backward(
        place,
        adapter_id,
        tokens,
        cotangent,
        again,
        mgain,
        (after, probs, qkv, weights, att, lows, wide),
        (sums[0].reshape(shape4), backs[0].reshape(shape4), pgrads[0].reshape(images, SEQ_PAD, 128)),
        (other, other, other_p),
        lefts,
        rights,
    )

    add = lambda a, b: (a.astype(F32) + b.astype(F32)).astype(BF16)
    grad = jnp.stack(grads)
    side = move(jnp.stack(sides), OVER_CORE)
    grad = jnp.concatenate([grad[..., :256, :], add(grad[..., 256:, :], side)], axis=3)
    half = G_ROWS // 2
    part_a, part_b = grad[..., :half, :], grad[..., half:, :]
    part_a = add(part_a[:, 0], move(part_a[:, 1], OVER_X))
    part_b = add(part_b[:, :, 0], move(part_b[:, :, 1], OVER_Y))
    part_a = add(part_a[:, 0], move(part_a[:, 1], OVER_Y))
    part_b = add(part_b[:, 0], move(part_b[:, 1], OVER_X))
    total = jnp.concatenate([part_a[0], part_b[0]], axis=0).astype(F32)
    joined = jnp.concatenate([part_a, part_b], axis=1)
    for ahead in range(1, PLANES):
        total = total + move(joined[ahead], to_plane(ahead)).astype(F32)
    dleft = total[0:128].T[None]
    uright = total[128:256][None]
    uleft = stacked_again(total[256:288]).T[None]
    dright = stacked_again(total[288:320])[None]

    left_parts = lgrad.reshape(640, 4, 128).transpose(1, 0, 2).reshape(4, 640 * 128)
    rq = rgrad.reshape(4, 4, 32, 512).transpose(1, 0, 2, 3).reshape(4, 4 * 32 * 512)
    rr = rright.reshape(4, 32 * 128)
    parts = jnp.concatenate([left_parts, rq, rr], axis=1).astype(BF16)
    parts = parts.reshape(2, 2, -1, 512)
    keep = lambda p, i, axis: lax.dynamic_index_in_dim(p, i, axis, keepdims=False)
    got = move(keep(parts, 1 - core, 1), OVER_CORE)
    parts = add(keep(parts, core, 1), got)
    got = move(keep(parts, 1 - row, 0), OVER_Y)
    part = add(keep(parts, row, 0), got)
    part = add(part, move(part, OVER_X))
    summed = part.astype(F32)
    for ahead in range(1, PLANES):
        summed = summed + move(part, to_plane(ahead)).astype(F32)
    summed = summed.reshape(-1)
    n1, n2 = 640 * 128, 4 * 32 * 512
    lsum = summed[:n1].reshape(640, 128)
    rsum = summed[n1 : n1 + n2].reshape(4, 32, 512)
    rrsum = summed[n1 + n2 :].reshape(32, 128)
    return (
        layer_out,
        tokens_grad,
        lsum[:384].T,
        rsum[:3],
        lsum[384:512].T,
        rsum[3],
        lsum[512:].T,
        rrsum[:, : router_right.shape[1]],
        uleft,
        uright,
        dleft,
        dright,
    )


def on_device(*arrays):
    sizes = (lax.axis_size("expert"), lax.axis_size("shard"))
    if sizes == (PLANES * COLS_X, ROWS_Y * CORES):
        return gathered_path(*arrays)
    return general_path(*arrays)


def solution(mesh):
    return jax.shard_map(
        on_device,
        mesh=mesh,
        in_specs=(
            P(("expert", "shard"), None, None),
            P(),
            P(),
            P("shard", None),
            P("shard", None),
            P("shard", None),
            P("expert", None, "shard"),
            P("expert", "shard", None),
            P("shard", None),
            P(None, "shard", None),
            P("shard", None),
            P("shard", None),
            P("shard", None),
            P("shard", None),
            P("expert", "shard", None),
            P("expert", None, "shard"),
            P("expert", "shard", None),
            P("expert", None, "shard"),
            P(("expert", "shard"), None, None),
            P(),
            P(("expert", "shard")),
            P(("expert", "shard"), None, None),
        ),
        out_specs=(
            P(("expert", "shard"), None, None),
            P(("expert", "shard"), None, None),
            P("shard", None),
            P(None, "shard", None),
            P("shard", None),
            P("shard", None),
            P("shard", None),
            P("shard", None),
            P("expert", "shard", None),
            P("expert", None, "shard"),
            P("expert", "shard", None),
            P("expert", None, "shard"),
        ),
        check_vma=False,
    )
```
